32 devices in a mesh: groups: 2 (over y), space: 4 (over z), mp: 2 (over x), sub: 2 (over core).
Axes of the slice: x: 2, y: 2, z: 4, core: 2. Of those that a mesh axis runs over, the one named last changes fastest.
Arguments:
- voxels: bfloat16 [24576, 512], P(('groups', 'space', 'sub')), parts along dimension 0, may hold values from -6 to 6
- window_ids: int32 [24576], P(('groups', 'space', 'sub')), parts along dimension 0, may hold values from 0 to 127, as said below
- voxel_slots: int32 [24576], P(('groups', 'space', 'sub')), parts along dimension 0, may hold values from 0 to 255, as said below
- window_counts: int32 [256], P('groups'), parts along dimension 0, may hold values from 0 to 256, as said below
- norm_gain: float32 [512], replicated, may hold values from 0.25 to 1.75
- w_query_key: bfloat16 [2, 512, 512], P(None, None, 'mp'), may hold values from -2 to 2
- w_value: bfloat16 [512, 512], P(None, 'mp'), may hold values from -0.25 to 0.25
- w_out: bfloat16 [512, 512], P('mp'), may hold values from -0.25 to 0.25
- ffn_gain: float32 [512], replicated, may hold values from 0.25 to 1.75
- w_up: bfloat16 [512, 2048], P(None, 'mp'), may hold values from -0.25 to 0.25
- w_down: bfloat16 [2048, 512], P('mp'), may hold values from -0.125 to 0.125
Outputs:
- result: bfloat16 [24576, 512], P(('groups', 'space', 'sub'), 'mp'), parts along dimension 0
The draws below stay inside these ranges and needn't reach their ends.
There are 2 independent parts, one for each index of `groups`. The reference program is written for one: setup_inputs(seed, part) draws one part's arguments, and reference() takes and returns one part's arrays. A program takes and returns all parts, laid end to end along the dimension named above; an argument that names none is the same for every part. Nothing has to cross between parts.
Inputs may be any that keep to these rules, and one draw needn't show every extreme that they name: `window_ids`: window w belongs to owner w // 16 (its index along space+sub) as that owner's window w % 16. On the voxels of one device at most 384 lie in windows of one owner, and in every draw some owner has exactly 384 voxels of every device. `voxel_slots`: the voxels of a window hold slots 0 to its count - 1, each once. window_counts[w] is the number of voxels with window id w; some window holds 256.
All inputs are finite; a program needn't handle non-finite values.
Results may differ from the reference program's by a relative error of at most 0.012.
Values may be sent and summed in bfloat16 or wider, within the bound.
A program may use at most 128 MiB of HBM per device.

```python
import jax
import jax.numpy as jnp
from jax import lax

D = 512
HEADS = 8
HDIM = 64
FF = 2048
WLEN = 256
VOX_DEV = 1536
NOWN = 8
VOX = 12288
CAP = 384
WIN_DEV = 16
NWIN = 128


def scene(key):
    owner_total = NOWN
    capacity = CAP
    per_owner = WIN_DEV
    key_bias = jax.random.fold_in(key, 101)
    key_first = jax.random.fold_in(key, 102)
    key_score = jax.random.fold_in(key, 103)
    key_shuffle = jax.random.fold_in(key, 104)
    key_sizes = jax.random.fold_in(key, 105)
    bias = jax.random.randint(key_bias, (owner_total,), 0, 3)
    busiest = jax.random.randint(key_first, (), 0, owner_total)
    bias = jnp.where(jnp.arange(owner_total) == busiest, 3, bias)
    scores = jax.random.randint(key_score, (owner_total, owner_total, capacity), 0, 1 << 20) + (bias * (1 << 20))[None, :, None]
    scores = scores.reshape(owner_total, owner_total * capacity)
    chosen = jnp.argsort(-scores, axis=1, stable=True)[:, :VOX_DEV].astype(jnp.int32)
    source_ids = jnp.arange(owner_total, dtype=jnp.int32)[:, None]
    selected = jnp.zeros((owner_total, owner_total * capacity), jnp.int32).at[source_ids, chosen].set(1)
    shuffles = jax.vmap(lambda sub_key: jax.random.permutation(sub_key, VOX_DEV))(jax.random.split(key_shuffle, owner_total))
    slot_ids = jnp.take_along_axis(chosen, shuffles.astype(jnp.int32), axis=1)
    owner_of = slot_ids // capacity
    column_of = slot_ids % capacity
    by_owner = selected.reshape(owner_total, owner_total, capacity).transpose(1, 0, 2).reshape(owner_total, owner_total * capacity)
    earlier = (jnp.cumsum(by_owner, axis=1) - by_owner).reshape(owner_total, owner_total, capacity)
    rank_of = earlier[owner_of, jnp.broadcast_to(source_ids, owner_of.shape), column_of]
    sizes = jax.random.randint(key_sizes, (owner_total, per_owner), 3 * WLEN // 4, WLEN + 1)
    sizes = sizes.at[:, 0].set(WLEN)
    ends = jnp.cumsum(sizes, axis=1)
    starts = ends - sizes
    local_win = jnp.sum((rank_of[:, :, None] >= ends[owner_of]).astype(jnp.int32), axis=-1)
    slot_in = rank_of - jnp.take_along_axis(starts[owner_of], local_win[:, :, None], axis=-1)[:, :, 0]
    load = jnp.sum(selected.reshape(owner_total, owner_total, capacity), axis=(0, 2))
    counts_flat = jnp.clip(load[:, None] - starts, 0, sizes).reshape(-1)
    window_of = owner_of * per_owner + local_win
    return (window_of.reshape(-1).astype(jnp.int32), slot_in.reshape(-1).astype(jnp.int32), counts_flat.astype(jnp.int32))


def draw_window_ids(key, part):
    return scene(key)[0]


def draw_voxel_slots(key, part):
    return scene(key)[1]


def draw_window_counts(key, part):
    return scene(key)[2]


def draw_w_query_key(key, part):
    key_base = jax.random.fold_in(key, 201)
    stacked = jax.random.normal(key_base, (2, D, D), jnp.float32) * D ** (-0.5)
    return jnp.clip(stacked, -2.0, 2.0).astype(jnp.bfloat16)


def block_scale(rng, dims, pieces, low, high):
    factor_of, own = 1.0, jax.random.fold_in(rng, 6)
    for axis_at, shards_of in pieces:
        heights = jnp.exp(jax.random.uniform(jax.random.fold_in(own, axis_at), (shards_of,), jnp.float32, low / len(pieces), high / len(pieces)))
        factor_of = factor_of * jnp.repeat(heights, dims[axis_at] // shards_of).reshape([-1 if axis == axis_at else 1 for axis in range(len(dims))])
    return factor_of


def scatter_about(stream_key, dims, deviation, limit, pieces=(), kind=jnp.bfloat16):
    values = jax.random.normal(stream_key, dims, jnp.float32) * deviation
    if len(pieces) > 0:
        values = block_scale(stream_key, dims, pieces, -0.22, 0.18) * values
    return jnp.clip(values, min=-limit, max=limit).astype(kind)


def setup_inputs(seed: int = 0, part: int = 0) -> dict:
    splits = jax.random.split(jax.random.key(seed), 12)
    part_splits = jax.random.split(jax.random.fold_in(splits[11], part), 12)
    voxels = scatter_about(part_splits[0], (VOX, D), 1.0, 6.0, ((0, 8),))
    window_ids = draw_window_ids(jax.random.fold_in(jax.random.fold_in(splits[11], part), 71), part)
    voxel_slots = draw_voxel_slots(jax.random.fold_in(jax.random.fold_in(splits[11], part), 71), part)
    window_counts = draw_window_counts(jax.random.fold_in(jax.random.fold_in(splits[11], part), 71), part)
    norm_gain = jnp.clip(1.0 + 0.15 * jax.random.normal(splits[4], (D,), jnp.float32), 0.25, 1.75)
    w_query_key = draw_w_query_key(jax.random.fold_in(splits[11], 71), part)
    w_value = scatter_about(splits[6], (D, D), D ** -0.5, 0.25, ((1, 2),))
    w_out = scatter_about(splits[7], (D, D), D ** -0.5, 0.25, ((0, 2),))
    ffn_gain = jnp.clip(1.0 + 0.15 * jax.random.normal(splits[8], (D,), jnp.float32), 0.25, 1.75)
    w_up = scatter_about(splits[9], (D, FF), D ** -0.5, 0.25, ((1, 2),))
    w_down = scatter_about(splits[10], (FF, D), FF ** -0.5, 0.125, ((0, 2),))
    return dict(voxels=voxels, window_ids=window_ids, voxel_slots=voxel_slots, window_counts=window_counts, norm_gain=norm_gain, w_query_key=w_query_key, w_value=w_value, w_out=w_out, ffn_gain=ffn_gain, w_up=w_up, w_down=w_down)


def normalize(values_in, gain):
    row_mean = lax.optimization_barrier(jnp.mean(values_in, axis=-1, keepdims=True))
    centred = values_in - row_mean
    variance = lax.optimization_barrier(jnp.mean(centred * centred, axis=-1, keepdims=True))
    return centred * lax.rsqrt(variance + 1e-05) * gain.astype(jnp.float32)

def reference(voxels, window_ids, voxel_slots, window_counts, norm_gain, w_query_key, w_value, w_out, ffn_gain, w_up, w_down):
    stream = voxels.astype(jnp.float32)
    normed = normalize(stream, norm_gain).astype(jnp.bfloat16)
    queries = jnp.dot(normed, w_query_key[0], preferred_element_type=jnp.float32).astype(jnp.bfloat16)
    key_rows = jnp.dot(normed, w_query_key[1], preferred_element_type=jnp.float32).astype(jnp.bfloat16)
    values = jnp.dot(normed, w_value, preferred_element_type=jnp.float32).astype(jnp.bfloat16)
    flat_index = (window_ids * WLEN + voxel_slots).astype(jnp.int32)
    slot_table = jnp.zeros((NWIN * WLEN,), jnp.int32).at[flat_index].set(jnp.arange(VOX, dtype=jnp.int32))
    slot_table = slot_table.reshape(NWIN, WLEN)

    def one_window(operands):
        members, count = operands
        split_shape = (WLEN, HEADS, HDIM)
        window_q = queries[members].astype(jnp.float32).reshape(split_shape)
        window_k = key_rows[members].astype(jnp.float32).reshape(split_shape)
        window_v = values[members].astype(jnp.float32).reshape(split_shape)
        scores = jnp.einsum('qhd,khd->hqk', window_q, window_k, precision=lax.Precision.HIGHEST) * HDIM ** (-0.5)
        live_keys = jnp.arange(WLEN, dtype=jnp.int32) < count
        scores = jnp.where(live_keys[None, None, :], scores, jnp.float32(-1e+30))
        row_max = lax.optimization_barrier(jnp.max(scores, axis=-1, keepdims=True))
        weights = jnp.exp(scores - row_max)
        probabilities = (weights / lax.optimization_barrier(jnp.sum(weights, axis=-1, keepdims=True))).astype(jnp.bfloat16)
        mixture = jnp.einsum('hqk,khd->qhd', probabilities.astype(jnp.float32), window_v, precision=lax.Precision.HIGHEST)
        return mixture.astype(jnp.bfloat16).reshape(WLEN, D)
    windows_out = lax.map(one_window, (slot_table, window_counts))
    attended = windows_out.reshape(NWIN * WLEN, D)[flat_index]
    after_attn = stream + jnp.dot(attended, w_out, preferred_element_type=jnp.float32)
    normed_ffn = normalize(after_attn, ffn_gain).astype(jnp.bfloat16)
    hidden = jax.nn.gelu(jnp.dot(normed_ffn, w_up, preferred_element_type=jnp.float32), approximate=True).astype(jnp.bfloat16)
    return (after_attn + jnp.dot(hidden, w_down, preferred_element_type=jnp.float32)).astype(jnp.bfloat16)
```

```python
import functools
import math

import jax
import jax.numpy as jnp
from jax import lax
from jax.experimental import pallas as pl
from jax.experimental.pallas import tpu as pltpu
from jax.sharding import PartitionSpec as P

HDIM = 64
WLEN = 256
WIN_DEV = 16
BASE = 64
SLOTS = WIN_DEV * WLEN
MESH = pl.DeviceIdType.MESH
VMEM = pl.BlockSpec(memory_space=pltpu.VMEM)
SMEM = pl.BlockSpec(memory_space=pltpu.SMEM)
ANY = pl.BlockSpec(memory_space=pl.ANY)
f32 = jnp.float32
bf16 = jnp.bfloat16


def normalize(values_in, gain):
    row_mean = jnp.mean(values_in, axis=-1, keepdims=True)
    centred = values_in - row_mean
    variance = jnp.mean(centred * centred, axis=-1, keepdims=True)
    return centred * lax.rsqrt(variance + 1e-05) * gain


def iota(shape, dim):
    return lax.broadcasted_iota(jnp.int32, shape, dim)


def one_hot(found):
    return jnp.where(found, f32(1), f32(0)).astype(bf16)


def dot(a, b, dims=((1,), (0,))):
    return lax.dot_general(a, b, (dims, ((), ())), preferred_element_type=f32)


def greet(owners, subs, mp_n, me, m):
    barrier = pltpu.get_barrier_semaphore()
    for k in range(1, owners):
        t = (me + k) % owners
        pl.semaphore_signal(
            barrier, inc=1, device_id={"space": t // subs, "sub": t % subs}, device_id_type=MESH
        )
    for p in range(1, mp_n):
        pl.semaphore_signal(
            barrier, inc=1, device_id={"mp": (m + p) % mp_n}, device_id_type=MESH
        )
    return lambda: pl.semaphore_wait(barrier, owners - 1 + mp_n - 1)


def remote(src, dst, sems, index, device):
    return pltpu.make_async_remote_copy(
        src_ref=src,
        dst_ref=dst,
        send_sem=sems[0].at[index],
        recv_sem=sems[1].at[index],
        device_id=device,
        device_id_type=MESH,
    )


def column_of(row):
    return jnp.transpose(jnp.broadcast_to(row, (128, row.shape[1])))


def widen(column, width):
    return jnp.concatenate([column] * (width // 128), axis=1)


def block_kernel(
    spaces, subs, mp_n, counts, ids, places, gain_in, gain_ffn, voxels, w_qk, w_v, w_out, w_up,
    w_down, result,
    normed, index, column, digits, outbuf, nearbuf, arrived, spotbuf, spots, posb, padded,
    qk, vv, mixture, total, outans, ansz, ansx, voxp, resout, resx, acc, kept, out_all, up_all, down_all,
    zs, zr, ps, pr, ss, sr, az, ar, bs, br, cs, cr, ws, wr, fs, fr, ls,
):
    owners = spaces * subs
    far = owners - subs
    sp, sb, m = lax.axis_index("space"), lax.axis_index("sub"), lax.axis_index("mp")
    me = sp * subs + sb
    cap, part = outbuf.shape[1], outbuf.shape[2]
    rows, width = normed.shape
    piece = cap // mp_n
    ready = greet(owners, subs, mp_n, me, m)

    local = [
        pltpu.make_async_copy(w_qk, qk, ls.at[0]),
        pltpu.make_async_copy(w_v, vv, ls.at[1]),
        pltpu.make_async_copy(w_out, out_all.at[m], ls.at[2]),
        pltpu.make_async_copy(w_up, up_all.at[m], ls.at[3]),
        pltpu.make_async_copy(w_down, down_all.at[m], ls.at[4]),
    ]
    for c in local:
        c.start()

    def share(ref, full, lo, hi):
        n = ref.shape[0] // subs // 2
        return [(ref, full, n * 2, lo * n, (hi - lo) * n)]

    first = share(w_out, out_all, 0, 2) + share(w_up, up_all, 0, 1)
    second = share(w_up, up_all, 1, 2) + share(w_down, down_all, 0, 2)

    def weight_copy(k, entry, p, h):
        ref, full, stride, lo, n = entry
        here = pl.ds(pl.multiple_of(sb * stride + lo, 16), n)
        return remote(
            ref.at[here], full.at[h, here], (ws, wr), k * mp_n + p, {"mp": (m + p) % mp_n}
        )

    def weight_pass(k, entry, p, u, h, owner_sb):
        _, full, stride, lo, n = entry
        here = pl.ds(pl.multiple_of(owner_sb * stride + lo, 16), n)
        return remote(
            full.at[h, here], full.at[h, here], (fs, fr), (k * mp_n + p) * subs + u,
            {"sub": (sb + u) % subs},
        )

    def weights_send(entries, base):
        for k, entry in enumerate(entries):
            for p in range(1, mp_n):
                weight_copy(base + k, entry, p, m).start()

    def weights_forward(entries, base):
        for k, entry in enumerate(entries):
            for p in range(1, mp_n):
                h = (m + mp_n - p) % mp_n
                weight_copy(base + k, entry, p, h).wait()
                for u in range(1, subs):
                    weight_pass(base + k, entry, p, u, h, sb).start()

    def weights_done(entries, base):
        for k, entry in enumerate(entries):
            for p in range(1, mp_n):
                h = (m + mp_n - p) % mp_n
                for u in range(1, subs):
                    weight_pass(base + k, entry, p, u, h, (sb + subs - u) % subs).wait()

    span = math.gcd(rows, 256)
    olanes = max(owners, 8)
    before_mask = one_hot(iota((span, span), 0) < iota((span, span), 1))
    carry = jnp.zeros((olanes, 1), f32)
    for c in range(rows // span):
        here = slice(c * span, (c + 1) * span)
        window = ids[:, here]
        destination = lax.shift_right_logical(window, WIN_DEV.bit_length() - 1)
        position = (window - destination * WIN_DEV) * WLEN + places[:, here]
        target = jnp.where(destination == iota((olanes, span), 0), f32(1), f32(0))
        before = dot(target.astype(bf16), before_mask) + carry
        carry = carry + jnp.sum(target, axis=1, keepdims=True)
        rank = jnp.sum(before * target, axis=0, keepdims=True).astype(jnp.int32)
        index[:, here] = destination * cap + rank
        high = lax.shift_right_logical(position, BASE.bit_length() - 1)
        row = iota((8, span), 0)
        digits[:, here] = jnp.where(
            row == 0, high, jnp.where(row == 1, position - high * BASE, jnp.where(row == 2, 1, 0))
        ).astype(f32).astype(bf16)

    lump = math.gcd(rows, 256)

    def norm_step(b, carry):
        here = pl.ds(pl.multiple_of(b * lump, lump), lump)
        normed[here, :] = normalize(voxels[here, :].astype(f32), gain_in[...]).astype(bf16)
        return carry

    lax.fori_loop(0, rows // lump, norm_step, 0)

    def sink(slot):
        return (sp + slot // subs + 1) % spaces * subs + (sb + slot % subs) % subs

    def source(slot):
        return (sp + spaces - slot // subs - 1) % spaces * subs + (sb + subs - slot % subs) % subs

    def owner_id(t):
        return {"space": t // subs, "sub": t % subs}

    def find(slot, t):
        hit = one_hot(index[...] == iota((cap, rows), 0) + t * cap)
        parts = dot(digits[...], hit, ((1,), (1,)))
        place = parts[0:1] * BASE + parts[1:2] + (1 - parts[2:3]) * SLOTS
        spotbuf[slot] = place.astype(jnp.int32)
        return hit

    def spot_copy(slot, s, t):
        return remote(spotbuf.at[slot], spots.at[s], (ps, pr), slot, owner_id(t))

    def far_copy(slot, s, t):
        return remote(outbuf.at[slot], arrived.at[s, m], (zs, zr), slot, owner_id(t))

    def near_copy(j, s, t):
        return remote(nearbuf.at[j], arrived.at[s], (zs, zr), far + j, owner_id(t))

    def side_copy(slot, p, half, s):
        return remote(
            arrived.at[s, m], arrived.at[s, half], (ss, sr), slot * mp_n + p,
            {"mp": (m + p) % mp_n},
        )

    def send(slot):
        far_copy(slot, me, sink(slot)).start()
        spot_copy(slot, me, sink(slot)).start()

    ready()

    def build(slot, carry):
        hit = find(slot, sink(slot))
        mine = normed[:, pl.ds(pl.multiple_of(m * part, part), part)]
        outbuf[slot] = dot(hit, mine).astype(bf16)

        @pl.when(slot > 0)
        def _():
            send(slot - 1)

        return carry

    lax.fori_loop(0, far, build, 0)
    weights_send(first, 0)
    for j in range(subs):
        hit = find(far + j, sp * subs + (sb + j) % subs)
        for h in range(mp_n):
            nearbuf[j, h] = dot(hit, normed[:, h * part : (h + 1) * part]).astype(bf16)
        if j == 0:
            send(far - 1)
        elif j > 1:
            near_copy(j - 1, me, sp * subs + (sb + j - 1) % subs).start()
            spot_copy(far + j - 1, me, sp * subs + (sb + j - 1) % subs).start()
    spots[me] = spotbuf[far]
    posb[me] = column_of(spotbuf[far])
    chunk = 4 * WLEN

    def put(s, blocks, first):
        row = spots[s]

        def step(c, carry):
            start = pl.multiple_of(c * chunk, chunk)
            hit = one_hot(row == iota((chunk, cap), 0) + start)
            here = pl.ds(start, chunk)
            for h in range(mp_n):
                new = dot(hit, blocks[h]).astype(bf16)
                if not first:
                    new += padded[here, h * part : (h + 1) * part]
                padded[here, h * part : (h + 1) * part] = new
            return carry

        lax.fori_loop(0, padded.shape[0] // chunk, step, 0)

    def pick_voxels(slot):
        s = sink(slot)
        hit = one_hot(index[...] == iota((piece, rows), 0) + (s * cap + m * piece))
        voxp[s] = dot(hit, voxels[...]).astype(bf16)

    put(me, nearbuf.at[0], True)
    for j in range(max(subs - 1, 1), subs):
        near_copy(j, me, sp * subs + (sb + j) % subs).start()
        spot_copy(far + j, me, sp * subs + (sb + j) % subs).start()
    column[...] = column_of(index[...])
    for j in range(subs):
        pick_voxels(far + j)

    def settle(slot):
        s = source(slot)
        for p in range(1, mp_n):
            side_copy(slot, p, (m + mp_n - p) % mp_n, s).wait()
        spot_copy(slot, s, s).wait()
        posb[s] = column_of(spots[s])
        put(s, arrived.at[s], False)

    def onward(slot, carry):
        s = source(slot)
        far_copy(slot, s, s).wait()
        for p in range(1, mp_n):
            side_copy(slot, p, m, s).start()

        @pl.when(slot > 0)
        def _():
            settle(slot - 1)

        pick_voxels(slot)
        return carry

    lax.fori_loop(0, far, onward, 0)
    weights_send(second, len(first))
    for j in range(1, subs):
        s = sp * subs + (sb + subs - j) % subs
        near_copy(j, s, s).wait()
        spot_copy(far + j, s, s).wait()
        posb[s] = column_of(spots[s])
        put(s, arrived.at[s], False)
    weights_forward(first, 0)
    settle(far - 1)
    for c in local:
        c.wait()

    group = 2
    heads = part // HDIM
    head_of = iota((1, part), 1) // HDIM
    masks = [one_hot(head_of == h) for h in range(heads)]

    def attend(step, carry):
        start = pl.multiple_of(step * group * WLEN, group * WLEN)
        here = pl.ds(start, group * WLEN)
        rows_in = padded[here, :]
        queries = dot(rows_in, qk[0]).astype(bf16)
        keys = dot(rows_in, qk[1]).astype(bf16)
        values = dot(rows_in, vv[...]).astype(bf16)
        for g in range(group):
            inner = slice(g * WLEN, (g + 1) * WLEN)
            q, k, v = queries[inner], keys[inner], values[inner]
            stacked = jnp.concatenate([q * masks[h] for h in range(heads)], axis=0)
            scores = dot(stacked, k, ((1,), (1,))) * f32(HDIM ** -0.5)
            live = iota((1, WLEN), 1) < counts[me * WIN_DEV + step * group + g]
            scores = jnp.where(live, scores, f32(-1e30))
            weights = jnp.exp(scores - jnp.max(scores, axis=-1, keepdims=True))
            scale = 1.0 / jnp.sum(weights, axis=-1, keepdims=True)
            mixed = dot((weights * scale).astype(bf16), v)
            out = mixed[:WLEN]
            for h in range(1, heads):
                out = jnp.where(head_of == h, mixed[h * WLEN : (h + 1) * WLEN], out)
            mixture[pl.ds(start + g * WLEN, WLEN), :] = out.astype(bf16)
        return carry

    lax.fori_loop(0, WIN_DEV // group, attend, 0)

    def answer_copy(slot, s, t):
        return remote(outans.at[slot], ansz.at[s], (az, ar), slot, owner_id(t))

    def gather(t):
        place = posb[t]
        total[...] = jnp.zeros_like(total)

        def add(c, inner):
            start = pl.multiple_of(c * chunk, chunk)
            hit = one_hot(widen(place, chunk) == iota((cap, chunk), 1) + start)
            total[...] += dot(hit, mixture[pl.ds(start, chunk), :])
            return inner

        lax.fori_loop(0, SLOTS // chunk, add, 0)

    def reply(slot, carry):
        gather(sink(slot))
        for h in range(mp_n):
            outans[slot, h] = total[h * piece : (h + 1) * piece, :].astype(bf16)

        @pl.when((slot > 0) & (slot != far + 1))
        def _():
            answer_copy(slot - 1, me, sink(slot - 1)).start()

        return carry

    lax.fori_loop(0, owners, reply, 0)
    if subs > 1:
        answer_copy(owners - 1, me, sink(owners - 1)).start()
    ansz[me] = outans[far]
    acc[...] = jnp.zeros_like(acc)
    weights_forward(second, len(first))
    weights_done(first, 0)
    weights_done(second, len(first))

    def slot_of(i):
        return (i + far) % owners

    def swap_copy(i, p, s, src_m):
        return remote(
            ansz.at[s, (m + p) % mp_n], ansx.at[src_m, s], (bs, br), i * mp_n + p,
            {"mp": (m + p) % mp_n},
        )

    def give_copy(i, p, s, src_m):
        return remote(
            resout.at[s, (m + p) % mp_n], resx.at[s, src_m], (cs, cr), i * mp_n + p,
            {"mp": (m + p) % mp_n},
        )

    def finish(i, carry):
        @pl.when(i < owners)
        def _():
            slot = slot_of(i)
            s = source(slot)

            @pl.when(i > 0)
            def _():
                answer_copy(slot, s, s).wait()

            for p in range(1, mp_n):
                swap_copy(i, p, s, m).start()
            ansx[m, s] = ansz[s, m]

        @pl.when((i > 0) & (i <= owners))
        def _():
            s = source(slot_of(i - 1))
            for p in range(1, mp_n):
                swap_copy(i - 1, p, s, (m + mp_n - p) % mp_n).wait()
            after = voxp[s].astype(f32)
            for h in range(mp_n):
                after += dot(ansx[h, s], out_all[h])
            ready_rows = normalize(after, gain_ffn[...]).astype(bf16)
            kept[...] = after
            terms = None
            for h in range(mp_n):
                hidden = jax.nn.gelu(dot(ready_rows, up_all[h]), approximate=True).astype(bf16)
                part_sum = dot(hidden, down_all[h])
                terms = part_sum if terms is None else terms + part_sum
            done = (kept[...] + terms).astype(bf16)
            for h in range(mp_n):
                resout[s, h] = done[:, h * part : (h + 1) * part]

        @pl.when(i > 1)
        def _():
            s = source(slot_of(i - 2))
            for p in range(1, mp_n):
                give_copy(i - 2, p, s, (m + mp_n - p) % mp_n).wait()
            hit = one_hot(widen(column[...], cap) == iota((rows, cap), 1) + s * cap)
            acc[...] += dot(hit, resx[s].reshape(cap, part))

        @pl.when((i > 0) & (i <= owners))
        def _():
            s = source(slot_of(i - 1))
            for p in range(1, mp_n):
                give_copy(i - 1, p, s, m).start()
            resx[s, m] = resout[s, m]

        return carry

    lax.fori_loop(0, owners + 2, finish, 0)
    result[...] = acc[...].astype(bf16)


def shards(
    subs,
    voxels,
    window_ids,
    voxel_slots,
    window_counts,
    norm_gain,
    w_query_key,
    w_value,
    w_out,
    ffn_gain,
    w_up,
    w_down,
):
    owners = lax.axis_size(("space", "sub"))
    mp_n = lax.axis_size("mp")
    rows, width = voxels.shape
    part = width // mp_n
    unit = math.lcm(128, 16 * mp_n)
    cap = -(-(2 * rows // owners) // unit) * unit
    piece = cap // mp_n
    far = owners - subs
    dma = pltpu.SemaphoreType.DMA
    i32 = jnp.int32
    pieces = 4 * mp_n
    return pl.pallas_call(
        functools.partial(block_kernel, owners // subs, subs, mp_n),
        out_shape=jax.ShapeDtypeStruct((rows, part), bf16),
        in_specs=[SMEM] + [VMEM] * 5 + [ANY] * 5,
        out_specs=VMEM,
        scratch_shapes=[
            pltpu.VMEM((rows, width), bf16),
            pltpu.VMEM((1, rows), i32),
            pltpu.VMEM((rows, 128), i32),
            pltpu.VMEM((8, rows), bf16),
            pltpu.VMEM((far, cap, part), bf16),
            pltpu.VMEM((subs, mp_n, cap, part), bf16),
            pltpu.VMEM((owners, mp_n, cap, part), bf16),
            pltpu.VMEM((owners, 1, cap), i32),
            pltpu.VMEM((owners, 1, cap), i32),
            pltpu.VMEM((owners, cap, 128), i32),
            pltpu.VMEM((SLOTS, width), bf16),
            pltpu.VMEM(w_query_key.shape, bf16),
            pltpu.VMEM(w_value.shape, bf16),
            pltpu.VMEM((SLOTS, part), bf16),
            pltpu.VMEM((cap, part), f32),
            pltpu.VMEM((owners, mp_n, piece, part), bf16),
            pltpu.VMEM((owners, mp_n, piece, part), bf16),
            pltpu.VMEM((mp_n, owners, piece, part), bf16),
            pltpu.VMEM((owners, piece, width), bf16),
            pltpu.VMEM((owners, mp_n, piece, part), bf16),
            pltpu.VMEM((owners, mp_n, piece, part), bf16),
            pltpu.VMEM((rows, part), f32),
            pltpu.VMEM((piece, width), f32),
            pltpu.VMEM((mp_n,) + w_out.shape, bf16),
            pltpu.VMEM((mp_n,) + w_up.shape, bf16),
            pltpu.VMEM((mp_n,) + w_down.shape, bf16),
            dma((owners,)), dma((owners,)), dma((owners,)), dma((owners,)),
            dma((far * mp_n,)), dma((far * mp_n,)),
            dma((owners,)), dma((owners,)),
            dma((owners * mp_n,)), dma((owners * mp_n,)),
            dma((owners * mp_n,)), dma((owners * mp_n,)),
            dma((pieces,)), dma((pieces,)),
            dma((pieces * subs,)), dma((pieces * subs,)),
            dma((5,)),
        ],
        compiler_params=pltpu.CompilerParams(
            collective_id=0, has_side_effects=True, vmem_limit_bytes=62 * 1024 * 1024
        ),
        name="block",
    )(
        window_counts, window_ids[None, :], voxel_slots[None, :], norm_gain[None, :],
        ffn_gain[None, :], voxels, w_query_key, w_value, w_out, w_up, w_down,
    )


def solution(mesh):
    return jax.shard_map(
        functools.partial(shards, mesh.shape["sub"]),
        mesh=mesh,
        in_specs=(
            P(("groups", "space", "sub"), None),
            P(("groups", "space", "sub")),
            P(("groups", "space", "sub")),
            P("groups"),
            P(),
            P(None, None, "mp"),
            P(None, "mp"),
            P("mp", None),
            P(),
            P(None, "mp"),
            P("mp", None),
        ),
        out_specs=P(("groups", "space", "sub"), "mp"),
        check_vma=False,
    )
```

```python
import functools
import math

import jax
import jax.numpy as jnp
from jax import lax
from jax.experimental import pallas as pl
from jax.experimental.pallas import tpu as pltpu
from jax.sharding import PartitionSpec as P

HDIM = 64
WLEN = 256
WIN_DEV = 16
BASE = 64
SLOTS = WIN_DEV * WLEN
MESH = pl.DeviceIdType.MESH
VMEM = pl.BlockSpec(memory_space=pltpu.VMEM)
SMEM = pl.BlockSpec(memory_space=pltpu.SMEM)
ANY = pl.BlockSpec(memory_space=pl.ANY)
f32 = jnp.float32
bf16 = jnp.bfloat16


def normalize(values_in, gain):
    row_mean = jnp.mean(values_in, axis=-1, keepdims=True)
    centred = values_in - row_mean
    variance = jnp.mean(centred * centred, axis=-1, keepdims=True)
    return centred * lax.rsqrt(variance + 1e-05) * gain


def iota(shape, dim):
    return lax.broadcasted_iota(jnp.int32, shape, dim)


def one_hot(found):
    return jnp.where(found, f32(1), f32(0)).astype(bf16)


def dot(a, b, dims=((1,), (0,))):
    return lax.dot_general(a, b, (dims, ((), ())), preferred_element_type=f32)


def greet(groups, spaces, subs, mp_n, g, sp, sb, m):
    barrier = pltpu.get_barrier_semaphore()
    everyone = spaces * subs * mp_n
    me = (sp * subs + sb) * mp_n + m
    for k in range(1, everyone):
        t = (me + k) % everyone
        pl.semaphore_signal(
            barrier,
            inc=1,
            device_id={"space": t // mp_n // subs, "sub": t // mp_n % subs, "mp": t % mp_n},
            device_id_type=MESH,
        )
    for k in range(1, groups):
        for u in range(subs):
            pl.semaphore_signal(
                barrier, inc=1, device_id={"groups": (g + k) % groups, "sub": u},
                device_id_type=MESH,
            )
    return lambda: pl.semaphore_wait(barrier, everyone - 1 + (groups - 1) * subs)


def remote(src, dst, sems, index, device):
    return pltpu.make_async_remote_copy(
        src_ref=src,
        dst_ref=dst,
        send_sem=sems[0].at[index],
        recv_sem=sems[1].at[index],
        device_id=device,
        device_id_type=MESH,
    )


def column_of(row):
    return jnp.transpose(jnp.broadcast_to(row, (128, row.shape[1])))


def widen(column, width):
    return jnp.concatenate([column] * (width // 128), axis=1)


def block_kernel(
    groups, spaces, subs, mp_n, counts, places, gain_in, gain_ffn, voxels, w_qk, w_v, w_out, w_up,
    w_down, result,
    normed, index, column, digits, outbuf, nearbuf, arrived, spotbuf, spots, posb, padded,
    qk, vv, mixture, total, outans, ansx, voxp, resout, resx, acc, kept, out_all, up_all, down_all,
    zs, zr, ns, nr, ps, pr, ss, sr, az, ar, cs, cr, ws, wr, fs, fr, ls,
):
    owners = spaces * subs
    far = owners - subs
    sp, sb, m = lax.axis_index("space"), lax.axis_index("sub"), lax.axis_index("mp")
    me = sp * subs + sb
    cap, part = outbuf.shape[1], outbuf.shape[2]
    rows, width = normed.shape
    piece = cap // mp_n
    g = lax.axis_index("groups")
    ready = greet(groups, spaces, subs, mp_n, g, sp, sb, m)

    local = [
        pltpu.make_async_copy(w_qk, qk, ls.at[0]),
        pltpu.make_async_copy(w_v, vv, ls.at[1]),
        pltpu.make_async_copy(w_out, out_all.at[m], ls.at[2]),
        pltpu.make_async_copy(w_up, up_all.at[m], ls.at[3]),
        pltpu.make_async_copy(w_down, down_all.at[m], ls.at[4]),
    ]
    for c in local:
        c.start()

    shares = groups * subs
    tables = ((w_out, out_all), (w_up, up_all), (w_down, down_all))

    def share_rows(ref, dg, du):
        n = ref.shape[0] // shares
        e = (g + dg) % groups * subs + (sb + du) % subs
        return pl.ds(pl.multiple_of(e * n, n), n)

    def weight_copy(k, p, h):
        ref, full = tables[k]
        here = share_rows(ref, 0, 0)
        return remote(
            ref.at[here], full.at[h, here], (ws, wr), k * mp_n + p, {"mp": (m + p) % mp_n}
        )

    def weight_pass(k, p, dg, du, h, back):
        ref, full = tables[k]
        here = share_rows(ref, groups - dg, subs - du) if back else share_rows(ref, 0, 0)
        return remote(
            full.at[h, here], full.at[h, here], (fs, fr),
            ((k * mp_n + p) * groups + dg) * subs + du,
            {"groups": (g + dg) % groups, "sub": (sb + du) % subs},
        )

    others = [(dg, du) for dg in range(groups) for du in range(subs) if dg + du > 0]

    def weights_send(which):
        for k in which:
            for p in range(1, mp_n):
                weight_copy(k, p, m).start()

    def weights_forward(which):
        for k in which:
            for p in range(1, mp_n):
                h = (m + mp_n - p) % mp_n
                weight_copy(k, p, h).wait()
                for dg, du in others:
                    weight_pass(k, p, dg, du, h, False).start()

    def weights_done():
        for k in range(3):
            for p in range(1, mp_n):
                for dg, du in others:
                    weight_pass(k, p, dg, du, (m + mp_n - p) % mp_n, True).wait()

    span = math.gcd(rows, 256)
    olanes = max(owners, 8)
    before_mask = one_hot(iota((span, span), 0) < iota((span, span), 1))
    carry = jnp.zeros((olanes, 1), f32)
    for c in range(rows // span):
        here = slice(c * span, (c + 1) * span)
        place = places[:, here]
        destination = lax.shift_right_logical(place, SLOTS.bit_length() - 1)
        position = place - destination * SLOTS
        target = jnp.where(destination == iota((olanes, span), 0), f32(1), f32(0))
        before = dot(target.astype(bf16), before_mask) + carry
        carry = carry + jnp.sum(target, axis=1, keepdims=True)
        rank = jnp.sum(before * target, axis=0, keepdims=True).astype(jnp.int32)
        index[:, here] = destination * cap + rank
        high = lax.shift_right_logical(position, BASE.bit_length() - 1)
        row = iota((8, span), 0)
        digits[:, here] = jnp.where(
            row == 0, high, jnp.where(row == 1, position - high * BASE, jnp.where(row == 2, 1, 0))
        ).astype(f32).astype(bf16)

    lump = math.gcd(rows, 256)

    def norm_step(b, carry):
        here = pl.ds(pl.multiple_of(b * lump, lump), lump)
        normed[here, :] = normalize(voxels[here, :].astype(f32), gain_in[...]).astype(bf16)
        return carry

    lax.fori_loop(0, rows // lump, norm_step, 0)

    def sink(slot):
        return (sp + slot // subs + 1) % spaces * subs + (sb + slot % subs) % subs

    def source(slot):
        return (sp + spaces - slot // subs - 1) % spaces * subs + (sb + subs - slot % subs) % subs

    def owner_id(t):
        return {"space": t // subs, "sub": t % subs}

    def find(slot, t):
        hit = one_hot(index[...] == iota((cap, rows), 0) + t * cap)
        parts = dot(digits[...], hit, ((1,), (1,)))
        place = parts[0:1] * BASE + parts[1:2] + (1 - parts[2:3]) * SLOTS
        spotbuf[slot] = place.astype(jnp.int32)
        return hit

    def slot_of(i):
        return (i + far) % owners

    def spot_copy(slot, s, t):
        return remote(spotbuf.at[slot], spots.at[s], (ps, pr), slot, owner_id(t))

    def part_rows(q):
        return pl.ds(q * piece, piece)

    def far_copy(slot, q, s, t):
        return remote(
            outbuf.at[slot, part_rows(q)], arrived.at[s, m, part_rows(q)], (zs, zr),
            slot * mp_n + q, owner_id(t),
        )

    def near_copy(slot, s, t):
        return remote(nearbuf.at[slot - far], arrived.at[s], (ns, nr), slot - far, owner_id(t))

    def side_copy(slot, q, p, half, s):
        return remote(
            arrived.at[s, m, part_rows(q)], arrived.at[s, half, part_rows(q)], (ss, sr),
            (slot * mp_n + q) * mp_n + p, {"mp": (m + p) % mp_n},
        )

    ready()

    def build(slot, carry):
        t = sink(slot)
        hit = one_hot(index[...] == iota((cap, rows), 0) + t * cap)
        mine = normed[:, pl.ds(pl.multiple_of(m * part, part), part)]
        outbuf[slot] = dot(hit, mine).astype(bf16)
        for q in range(mp_n):
            far_copy(slot, q, me, t).start()
        return carry

    lax.fori_loop(0, far, build, 0)
    weights_send((0, 1))

    def near_build():
        for j in range(subs):
            t = sink(far + j)
            hit = find(far + j, t)
            for h in range(mp_n):
                packed = dot(hit, normed[:, h * part : (h + 1) * part]).astype(bf16)
                if j == 0:
                    arrived[me, h] = packed
                else:
                    nearbuf[j, h] = packed
            if j == 0:
                spots[me] = spotbuf[far]
            else:
                near_copy(far + j, me, t).start()
                spot_copy(far + j, me, t).start()

    chunk = 4 * WLEN

    def put(base, first):
        row = jnp.concatenate([spots[base + u] for u in range(subs)], axis=1)

        def step(c, carry):
            start = pl.multiple_of(c * chunk, chunk)
            hit = one_hot(row == iota((chunk, subs * cap), 0) + start)
            here = pl.ds(start, chunk)
            for h in range(mp_n):
                block = arrived[pl.ds(base, subs), h].reshape(subs * cap, part)
                new = dot(hit, block).astype(bf16)
                if not first:
                    new += padded[here, h * part : (h + 1) * part]
                padded[here, h * part : (h + 1) * part] = new
            return carry

        lax.fori_loop(0, padded.shape[0] // chunk, step, 0)

    def pick_voxels(slot):
        s = sink(slot)
        hit = one_hot(index[...] == iota((piece, rows), 0) + (s * cap + m * piece))
        voxp[s] = dot(hit, voxels[...]).astype(bf16)

    def settle_near():
        for u in range(1, subs):
            s = source(far + u)
            near_copy(far + u, s, s).wait()
            spot_copy(far + u, s, s).wait()
        for u in range(subs):
            posb[sp * subs + u] = column_of(spots[sp * subs + u])
        put(sp * subs, True)

    def settle(chip):
        base = source(chip * subs) // subs * subs
        for u in range(subs):
            slot = chip * subs + u
            s = source(slot)
            for q in range(mp_n):
                for p in range(1, mp_n):
                    side_copy(slot, q, p, (m + mp_n - p) % mp_n, s).wait()
            spot_copy(slot, s, s).wait()
            posb[s] = column_of(spots[s])
        put(base, False)

    def onward(slot, carry):
        s = source(slot)
        for q in range(mp_n):
            far_copy(slot, q, s, s).wait()
            for p in range(1, mp_n):
                side_copy(slot, q, p, m, s).start()
        @pl.when(slot == 0)
        def _():
            near_build()
            column[...] = column_of(index[...])

        t = sink(slot)
        find(slot, t)
        pick_voxels(slot)
        spot_copy(slot, me, t).start()

        @pl.when(slot == subs - 1)
        def _():
            settle_near()

        @pl.when((slot > subs - 1) & (slot % subs == subs - 1))
        def _():
            settle(slot // subs - 1)

        return carry

    lax.fori_loop(0, far, onward, 0)
    weights_forward((0, 1))
    weights_send((2,))
    for j in range(subs):
        pick_voxels(far + j)
    settle(spaces - 2)
    for c in local:
        c.wait()

    group = 2
    heads = part // HDIM
    head_of = iota((1, part), 1) // HDIM
    masks = [one_hot(head_of == h) for h in range(heads)]

    def attend(step, carry):
        @pl.when(step == WIN_DEV // group * 3 // 4)
        def _():
            weights_forward((2,))

        start = pl.multiple_of(step * group * WLEN, group * WLEN)
        here = pl.ds(start, group * WLEN)
        rows_in = padded[here, :]
        queries = dot(rows_in, qk[0]).astype(bf16) * bf16(HDIM ** -0.5)
        keys = dot(rows_in, qk[1]).astype(bf16)
        values = dot(rows_in, vv[...]).astype(bf16)
        for g in range(group):
            inner = slice(g * WLEN, (g + 1) * WLEN)
            q, k, v = queries[inner], keys[inner], values[inner]
            stacked = jnp.concatenate([q * masks[h] for h in range(heads)], axis=0)
            scores = dot(stacked, k, ((1,), (1,)))
            live = iota((1, WLEN), 1) < counts[me * WIN_DEV + step * group + g]
            scores = jnp.where(live, scores, f32(-1e30))
            weights = jnp.exp(scores - jnp.max(scores, axis=-1, keepdims=True))
            scale = 1.0 / jnp.sum(weights, axis=-1, keepdims=True)
            mixed = dot(weights.astype(bf16), v)
            out = mixed[:WLEN] * scale[:WLEN]
            for h in range(1, heads):
                rows_h = slice(h * WLEN, (h + 1) * WLEN)
                out = jnp.where(head_of == h, mixed[rows_h] * scale[rows_h], out)
            mixture[pl.ds(start + g * WLEN, WLEN), :] = out.astype(bf16)
        return carry

    lax.fori_loop(0, WIN_DEV // group, attend, 0)

    def answer_copy(slot, d, s, t, src_m):
        target = {**owner_id(t), "mp": (m + d) % mp_n}
        return remote(
            outans.at[slot, (m + d) % mp_n], ansx.at[src_m, s], (az, ar), slot * mp_n + d, target
        )

    def gather(t):
        place = posb[t]
        total[...] = jnp.zeros_like(total)

        def add(c, inner):
            start = pl.multiple_of(c * chunk, chunk)
            hit = one_hot(widen(place, chunk) == iota((cap, chunk), 1) + start)
            total[...] += dot(hit, mixture[pl.ds(start, chunk), :])
            return inner

        lax.fori_loop(0, SLOTS // chunk, add, 0)

    def reply(r, carry):
        slot = jnp.where(r < subs, r, jnp.where(r < 2 * subs, far + r - subs, r - subs))
        t = sink(slot)
        gather(t)
        for h in range(mp_n):
            outans[slot, h] = total[h * piece : (h + 1) * piece, :].astype(bf16)
        for d in range(1, mp_n):
            answer_copy(slot, d, me, t, m).start()

        @pl.when(slot != far)
        def _():
            answer_copy(slot, 0, me, t, m).start()

        return carry

    lax.fori_loop(0, owners, reply, 0)
    ansx[m, me] = outans[far, m]
    acc[...] = jnp.zeros_like(acc)
    weights_done()

    def give_copy(i, p, s, src_m):
        return remote(
            resout.at[s, (m + p) % mp_n], resx.at[s, src_m], (cs, cr), i * mp_n + p,
            {"mp": (m + p) % mp_n},
        )

    def finish(i, carry):
        @pl.when(i < owners)
        def _():
            slot = slot_of(i)
            s = source(slot)
            for d in range(1, mp_n):
                answer_copy(slot, d, s, s, (m + mp_n - d) % mp_n).wait()

            @pl.when(i > 0)
            def _():
                answer_copy(slot, 0, s, s, m).wait()

            after = voxp[s].astype(f32)
            for h in range(mp_n):
                after += dot(ansx[h, s], out_all[h])
            ready_rows = normalize(after, gain_ffn[...]).astype(bf16)
            kept[...] = after
            terms = None
            for h in range(mp_n):
                hidden = jax.nn.gelu(dot(ready_rows, up_all[h]), approximate=True).astype(bf16)
                part_sum = dot(hidden, down_all[h])
                terms = part_sum if terms is None else terms + part_sum
            done = (kept[...] + terms).astype(bf16)
            for h in range(mp_n):
                resout[s, h] = done[:, h * part : (h + 1) * part]

        @pl.when(i > 1)
        def _():
            s = source(slot_of(i - 2))
            for p in range(1, mp_n):
                give_copy(i - 2, p, s, (m + mp_n - p) % mp_n).wait()
            hit = one_hot(widen(column[...], cap) == iota((rows, cap), 1) + s * cap)
            acc[...] += dot(hit, resx[s].reshape(cap, part))

        @pl.when(i < owners)
        def _():
            s = source(slot_of(i))
            for p in range(1, mp_n):
                give_copy(i, p, s, m).start()
            resx[s, m] = resout[s, m]

        return carry

    lax.fori_loop(0, owners + 2, finish, 0)
    result[...] = acc[...].astype(bf16)


def shards(
    subs,
    voxels,
    window_ids,
    voxel_slots,
    window_counts,
    norm_gain,
    w_query_key,
    w_value,
    w_out,
    ffn_gain,
    w_up,
    w_down,
):
    groups = lax.axis_size("groups")
    owners = lax.axis_size(("space", "sub"))
    mp_n = lax.axis_size("mp")
    rows, width = voxels.shape
    part = width // mp_n
    unit = math.lcm(128, 16 * mp_n)
    cap = -(-(2 * rows // owners) // unit) * unit
    piece = cap // mp_n
    far = owners - subs
    dma = pltpu.SemaphoreType.DMA
    i32 = jnp.int32
    pieces = 3 * mp_n
    return pl.pallas_call(
        functools.partial(block_kernel, groups, owners // subs, subs, mp_n),
        out_shape=jax.ShapeDtypeStruct((rows, part), bf16),
        in_specs=[SMEM] + [VMEM] * 4 + [ANY] * 5,
        out_specs=VMEM,
        scratch_shapes=[
            pltpu.VMEM((rows, width), bf16),
            pltpu.VMEM((1, rows), i32),
            pltpu.VMEM((rows, 128), i32),
            pltpu.VMEM((8, rows), bf16),
            pltpu.VMEM((far, cap, part), bf16),
            pltpu.VMEM((subs, mp_n, cap, part), bf16),
            pltpu.VMEM((owners, mp_n, cap, part), bf16),
            pltpu.VMEM((owners, 1, cap), i32),
            pltpu.VMEM((owners, 1, cap), i32),
            pltpu.VMEM((owners, cap, 128), i32),
            pltpu.VMEM((SLOTS, width), bf16),
            pltpu.VMEM(w_query_key.shape, bf16),
            pltpu.VMEM(w_value.shape, bf16),
            pltpu.VMEM((SLOTS, part), bf16),
            pltpu.VMEM((cap, part), f32),
            pltpu.VMEM((owners, mp_n, piece, part), bf16),
            pltpu.VMEM((mp_n, owners, piece, part), bf16),
            pltpu.VMEM((owners, piece, width), bf16),
            pltpu.VMEM((owners, mp_n, piece, part), bf16),
            pltpu.VMEM((owners, mp_n, piece, part), bf16),
            pltpu.VMEM((rows, part), f32),
            pltpu.VMEM((piece, width), f32),
            pltpu.VMEM((mp_n,) + w_out.shape, bf16),
            pltpu.VMEM((mp_n,) + w_up.shape, bf16),
            pltpu.VMEM((mp_n,) + w_down.shape, bf16),
            dma((far * mp_n,)), dma((far * mp_n,)), dma((subs,)), dma((subs,)),
            dma((owners,)), dma((owners,)),
            dma((far * mp_n * mp_n,)), dma((far * mp_n * mp_n,)),
            dma((owners * mp_n,)), dma((owners * mp_n,)),
            dma((owners * mp_n,)), dma((owners * mp_n,)),
            dma((pieces,)), dma((pieces,)),
            dma((pieces * groups * subs,)), dma((pieces * groups * subs,)),
            dma((5,)),
        ],
        compiler_params=pltpu.CompilerParams(
            collective_id=0, has_side_effects=True, vmem_limit_bytes=62 * 1024 * 1024
        ),
        name="block",
    )(
        window_counts, (window_ids * WLEN + voxel_slots)[None, :], norm_gain[None, :],
        ffn_gain[None, :], voxels, w_query_key, w_value, w_out, w_up, w_down,
    )


def solution(mesh):
    return jax.shard_map(
        functools.partial(shards, mesh.shape["sub"]),
        mesh=mesh,
        in_specs=(
            P(("groups", "space", "sub"), None),
            P(("groups", "space", "sub")),
            P(("groups", "space", "sub")),
            P("groups"),
            P(),
            P(None, None, "mp"),
            P(None, "mp"),
            P("mp", None),
            P(),
            P(None, "mp"),
            P("mp", None),
        ),
        out_specs=P(("groups", "space", "sub"), "mp"),
        check_vma=False,
    )
```

```python
import functools
import math

import jax
import jax.numpy as jnp
from jax import lax
from jax.experimental import pallas as pl
from jax.experimental.pallas import tpu as pltpu
from jax.sharding import PartitionSpec as P

HDIM = 64
WLEN = 256
WIN_DEV = 16
BASE = 64
SLOTS = WIN_DEV * WLEN
MESH = pl.DeviceIdType.MESH
VMEM = pl.BlockSpec(memory_space=pltpu.VMEM)
SMEM = pl.BlockSpec(memory_space=pltpu.SMEM)
ANY = pl.BlockSpec(memory_space=pl.ANY)
f32 = jnp.float32
bf16 = jnp.bfloat16


def normalize(values_in, gain):
    row_mean = jnp.mean(values_in, axis=-1, keepdims=True)
    centred = values_in - row_mean
    variance = jnp.mean(centred * centred, axis=-1, keepdims=True)
    return centred * lax.rsqrt(variance + 1e-05) * gain


def iota(shape, dim):
    return lax.broadcasted_iota(jnp.int32, shape, dim)


def one_hot(found):
    return jnp.where(found, f32(1), f32(0)).astype(bf16)


def dot(a, b, dims=((1,), (0,))):
    return lax.dot_general(a, b, (dims, ((), ())), preferred_element_type=f32)


def greet(groups, spaces, subs, mp_n, g, sp, sb, m):
    barrier = pltpu.get_barrier_semaphore()
    everyone = spaces * subs * mp_n
    me = (sp * subs + sb) * mp_n + m
    for k in range(1, everyone):
        t = (me + k) % everyone
        pl.semaphore_signal(
            barrier,
            inc=1,
            device_id={"space": t // mp_n // subs, "sub": t // mp_n % subs, "mp": t % mp_n},
            device_id_type=MESH,
        )
    for k in range(1, groups):
        for u in range(subs):
            pl.semaphore_signal(
                barrier, inc=1, device_id={"groups": (g + k) % groups, "sub": u},
                device_id_type=MESH,
            )
    return lambda: pl.semaphore_wait(barrier, everyone - 1 + (groups - 1) * subs)


def remote(src, dst, sems, index, device):
    return pltpu.make_async_remote_copy(
        src_ref=src,
        dst_ref=dst,
        send_sem=sems[0].at[index],
        recv_sem=sems[1].at[index],
        device_id=device,
        device_id_type=MESH,
    )


def column_of(row):
    return jnp.transpose(jnp.broadcast_to(row, (128, row.shape[1])))


def widen(column, width):
    return jnp.concatenate([column] * (width // 128), axis=1)


def block_kernel(
    groups, spaces, subs, mp_n, counts, places, gain_in, gain_ffn, voxels, w_qk, w_v, w_out, w_up,
    w_down, result,
    normed, index, column, digits, outbuf, nearbuf, arrived, spotbuf, spots, posb, padded,
    qk, vv, mixture, total, outans, ansx, voxp, resout, resx, acc, kept, out_all, up_all, down_all,
    zs, zr, ns, nr, ps, pr, ss, sr, az, ar, cs, cr, ws, wr, fs, fr, ls,
):
    owners = spaces * subs
    far = owners - subs
    sp, sb, m = lax.axis_index("space"), lax.axis_index("sub"), lax.axis_index("mp")
    me = sp * subs + sb
    cap, part = outbuf.shape[1], outbuf.shape[2]
    rows, width = normed.shape
    piece = cap // mp_n
    g = lax.axis_index("groups")
    ready = greet(groups, spaces, subs, mp_n, g, sp, sb, m)

    local = [
        pltpu.make_async_copy(w_qk, qk, ls.at[0]),
        pltpu.make_async_copy(w_v, vv, ls.at[1]),
        pltpu.make_async_copy(w_out, out_all.at[m], ls.at[2]),
        pltpu.make_async_copy(w_up, up_all.at[m], ls.at[3]),
        pltpu.make_async_copy(w_down, down_all.at[m], ls.at[4]),
    ]
    for c in local:
        c.start()

    shares = groups * subs
    tables = ((w_out, out_all), (w_up, up_all), (w_down, down_all))

    def share_rows(ref, dg, du):
        n = ref.shape[0] // shares
        e = (g + dg) % groups * subs + (sb + du) % subs
        return pl.ds(pl.multiple_of(e * n, n), n)

    def weight_copy(k, p, h):
        ref, full = tables[k]
        here = share_rows(ref, 0, 0)
        return remote(
            ref.at[here], full.at[h, here], (ws, wr), k * mp_n + p, {"mp": (m + p) % mp_n}
        )

    def weight_pass(k, p, dg, du, h, back):
        ref, full = tables[k]
        here = share_rows(ref, groups - dg, subs - du) if back else share_rows(ref, 0, 0)
        return remote(
            full.at[h, here], full.at[h, here], (fs, fr),
            ((k * mp_n + p) * groups + dg) * subs + du,
            {"groups": (g + dg) % groups, "sub": (sb + du) % subs},
        )

    others = [(dg, du) for dg in range(groups) for du in range(subs) if dg + du > 0]

    def weights_send(which):
        for k in which:
            for p in range(1, mp_n):
                weight_copy(k, p, m).start()

    def weights_forward(which):
        for k in which:
            for p in range(1, mp_n):
                h = (m + mp_n - p) % mp_n
                weight_copy(k, p, h).wait()
                for dg, du in others:
                    weight_pass(k, p, dg, du, h, False).start()

    def weights_done():
        for k in range(3):
            for p in range(1, mp_n):
                for dg, du in others:
                    weight_pass(k, p, dg, du, (m + mp_n - p) % mp_n, True).wait()

    span = math.gcd(rows, 256)
    olanes = max(owners, 8)
    before_mask = one_hot(iota((span, span), 0) < iota((span, span), 1))
    carry = jnp.zeros((olanes, 1), f32)
    for c in range(rows // span):
        here = slice(c * span, (c + 1) * span)
        place = jnp.concatenate(
            [places[r : r + 1, :] for r in range(here.start // 128, here.stop // 128)], axis=1
        )
        destination = lax.shift_right_logical(place, SLOTS.bit_length() - 1)
        position = place - destination * SLOTS
        target = jnp.where(destination == iota((olanes, span), 0), f32(1), f32(0))
        before = dot(target.astype(bf16), before_mask) + carry
        carry = carry + jnp.sum(target, axis=1, keepdims=True)
        rank = jnp.sum(before * target, axis=0, keepdims=True).astype(jnp.int32)
        index[:, here] = destination * cap + rank
        high = lax.shift_right_logical(position, BASE.bit_length() - 1)
        row = iota((8, span), 0)
        digits[:, here] = jnp.where(
            row == 0, high, jnp.where(row == 1, position - high * BASE, jnp.where(row == 2, 1, 0))
        ).astype(f32).astype(bf16)

    lump = math.gcd(rows, 256)

    def norm_step(b, carry):
        here = pl.ds(pl.multiple_of(b * lump, lump), lump)
        normed[here, :] = normalize(voxels[here, :].astype(f32), gain_in[...]).astype(bf16)
        return carry

    lax.fori_loop(0, rows // lump, norm_step, 0)

    def sink(slot):
        return (sp + slot // subs + 1) % spaces * subs + (sb + slot % subs) % subs

    def source(slot):
        return (sp + spaces - slot // subs - 1) % spaces * subs + (sb + subs - slot % subs) % subs

    def owner_id(t):
        return {"space": t // subs, "sub": t % subs}

    def find(slot, t):
        hit = one_hot(index[...] == iota((cap, rows), 0) + t * cap)
        parts = dot(digits[...], hit, ((1,), (1,)))
        place = parts[0:1] * BASE + parts[1:2] + (1 - parts[2:3]) * SLOTS
        spotbuf[slot] = place.astype(jnp.int32)
        return hit

    def slot_of(i):
        return (i + far) % owners

    def spot_copy(slot, s, t):
        return remote(spotbuf.at[slot], spots.at[s], (ps, pr), slot, owner_id(t))

    def part_rows(q):
        return pl.ds(q * piece, piece)

    def far_copy(slot, q, s, t):
        return remote(
            outbuf.at[slot, part_rows(q)], arrived.at[s, m, part_rows(q)], (zs, zr),
            slot * mp_n + q, owner_id(t),
        )

    def near_copy(slot, s, t):
        return remote(nearbuf.at[slot - far], arrived.at[s], (ns, nr), slot - far, owner_id(t))

    def side_copy(slot, q, p, half, s):
        return remote(
            arrived.at[s, m, part_rows(q)], arrived.at[s, half, part_rows(q)], (ss, sr),
            (slot * mp_n + q) * mp_n + p, {"mp": (m + p) % mp_n},
        )

    ready()

    def build(slot, carry):
        t = sink(slot)
        hit = one_hot(index[...] == iota((cap, rows), 0) + t * cap)
        mine = normed[:, pl.ds(pl.multiple_of(m * part, part), part)]
        outbuf[slot] = dot(hit, mine).astype(bf16)
        for q in range(mp_n):
            far_copy(slot, q, me, t).start()
        return carry

    lax.fori_loop(0, far, build, 0)
    weights_send((0, 1))

    def near_build():
        for j in range(subs):
            t = sink(far + j)
            hit = find(far + j, t)
            for h in range(mp_n):
                packed = dot(hit, normed[:, h * part : (h + 1) * part]).astype(bf16)
                if j == 0:
                    arrived[me, h] = packed
                else:
                    nearbuf[j, h] = packed
            if j == 0:
                spots[me] = spotbuf[far]
            else:
                near_copy(far + j, me, t).start()
                spot_copy(far + j, me, t).start()

    chunk = 4 * WLEN

    def put(base, first):
        row = jnp.concatenate([spots[base + u] for u in range(subs)], axis=1)

        def step(c, carry):
            start = pl.multiple_of(c * chunk, chunk)
            hit = one_hot(row == iota((chunk, subs * cap), 0) + start)
            here = pl.ds(start, chunk)
            for h in range(mp_n):
                block = arrived[pl.ds(base, subs), h].reshape(subs * cap, part)
                new = dot(hit, block).astype(bf16)
                if not first:
                    new += padded[here, h * part : (h + 1) * part]
                padded[here, h * part : (h + 1) * part] = new
            return carry

        lax.fori_loop(0, padded.shape[0] // chunk, step, 0)

    def pick_voxels(slot):
        s = sink(slot)
        hit = one_hot(index[...] == iota((piece, rows), 0) + (s * cap + m * piece))
        voxp[s] = dot(hit, voxels[...]).astype(bf16)

    def settle_near():
        for u in range(1, subs):
            s = source(far + u)
            near_copy(far + u, s, s).wait()
            spot_copy(far + u, s, s).wait()
        for u in range(subs):
            posb[sp * subs + u] = column_of(spots[sp * subs + u])
        put(sp * subs, True)

    def settle(chip):
        base = source(chip * subs) // subs * subs
        for u in range(subs):
            slot = chip * subs + u
            s = source(slot)
            for q in range(mp_n):
                for p in range(1, mp_n):
                    side_copy(slot, q, p, (m + mp_n - p) % mp_n, s).wait()
            spot_copy(slot, s, s).wait()
            posb[s] = column_of(spots[s])
        put(base, False)

    def onward(slot, carry):
        s = source(slot)
        for q in range(mp_n):
            far_copy(slot, q, s, s).wait()
            for p in range(1, mp_n):
                side_copy(slot, q, p, m, s).start()
        @pl.when(slot == 0)
        def _():
            near_build()
            column[...] = column_of(index[...])

        t = sink(slot)
        find(slot, t)
        pick_voxels(slot)
        spot_copy(slot, me, t).start()

        @pl.when(slot == subs - 1)
        def _():
            settle_near()

        @pl.when((slot > subs - 1) & (slot % subs == subs - 1))
        def _():
            settle(slot // subs - 1)

        return carry

    lax.fori_loop(0, far, onward, 0)
    weights_forward((0, 1))
    weights_send((2,))
    for j in range(subs):
        pick_voxels(far + j)
    settle(spaces - 2)
    for c in local:
        c.wait()

    group = 4
    heads = part // HDIM
    head_of = iota((1, part), 1) // HDIM
    masks = [one_hot(head_of == h) for h in range(heads)]

    def attend(step, carry):
        @pl.when(step == WIN_DEV // group * 3 // 4)
        def _():
            weights_forward((2,))

        start = pl.multiple_of(step * group * WLEN, group * WLEN)
        here = pl.ds(start, group * WLEN)
        rows_in = padded[here, :]
        queries = dot(rows_in, qk[0]).astype(bf16) * bf16(HDIM ** -0.5)
        keys = dot(rows_in, qk[1]).astype(bf16)
        values = dot(rows_in, vv[...]).astype(bf16)
        for g in range(group):
            inner = slice(g * WLEN, (g + 1) * WLEN)
            q, k, v = queries[inner], keys[inner], values[inner]
            stacked = jnp.concatenate([q * masks[h] for h in range(heads)], axis=0)
            scores = dot(stacked, k, ((1,), (1,)))
            live = iota((1, WLEN), 1) < counts[me * WIN_DEV + step * group + g]
            scores = jnp.where(live, scores, f32(-1e30))
            weights = jnp.exp(scores - jnp.max(scores, axis=-1, keepdims=True))
            scale = 1.0 / jnp.sum(weights, axis=-1, keepdims=True)
            mixed = dot(weights.astype(bf16), v)
            out = mixed[:WLEN] * scale[:WLEN]
            for h in range(1, heads):
                rows_h = slice(h * WLEN, (h + 1) * WLEN)
                out = jnp.where(head_of == h, mixed[rows_h] * scale[rows_h], out)
            mixture[pl.ds(start + g * WLEN, WLEN), :] = out.astype(bf16)
        return carry

    lax.fori_loop(0, WIN_DEV // group, attend, 0)

    def answer_copy(slot, d, s, t, src_m):
        target = {**owner_id(t), "mp": (m + d) % mp_n}
        return remote(
            outans.at[slot, (m + d) % mp_n], ansx.at[src_m, s], (az, ar), slot * mp_n + d, target
        )

    def gather(t):
        place = posb[t]
        total[...] = jnp.zeros_like(total)

        def add(c, inner):
            start = pl.multiple_of(c * chunk, chunk)
            hit = one_hot(widen(place, chunk) == iota((cap, chunk), 1) + start)
            total[...] += dot(hit, mixture[pl.ds(start, chunk), :])
            return inner

        lax.fori_loop(0, SLOTS // chunk, add, 0)

    def reply(r, carry):
        slot = jnp.where(r < subs, r, jnp.where(r < 2 * subs, far + r - subs, r - subs))
        t = sink(slot)
        gather(t)
        for h in range(mp_n):
            outans[slot, h] = total[h * piece : (h + 1) * piece, :].astype(bf16)
        for d in range(1, mp_n):
            answer_copy(slot, d, me, t, m).start()

        @pl.when(slot != far)
        def _():
            answer_copy(slot, 0, me, t, m).start()

        return carry

    lax.fori_loop(0, owners, reply, 0)
    ansx[m, me] = outans[far, m]
    acc[...] = jnp.zeros_like(acc)
    weights_done()

    def give_copy(i, p, s, src_m):
        return remote(
            resout.at[s, (m + p) % mp_n], resx.at[s, src_m], (cs, cr), i * mp_n + p,
            {"mp": (m + p) % mp_n},
        )

    def finish(i, carry):
        @pl.when(i < owners)
        def _():
            slot = slot_of(i)
            s = source(slot)
            for d in range(1, mp_n):
                answer_copy(slot, d, s, s, (m + mp_n - d) % mp_n).wait()

            @pl.when(i > 0)
            def _():
                answer_copy(slot, 0, s, s, m).wait()

            after = voxp[s].astype(f32)
            for h in range(mp_n):
                after += dot(ansx[h, s], out_all[h])
            ready_rows = normalize(after, gain_ffn[...]).astype(bf16)
            kept[...] = after
            terms = None
            for h in range(mp_n):
                hidden = jax.nn.gelu(dot(ready_rows, up_all[h]), approximate=True).astype(bf16)
                part_sum = dot(hidden, down_all[h])
                terms = part_sum if terms is None else terms + part_sum
            done = (kept[...] + terms).astype(bf16)
            for h in range(mp_n):
                resout[s, h] = done[:, h * part : (h + 1) * part]

        @pl.when(i > 1)
        def _():
            s = source(slot_of(i - 2))
            for p in range(1, mp_n):
                give_copy(i - 2, p, s, (m + mp_n - p) % mp_n).wait()
            hit = one_hot(widen(column[...], cap) == iota((rows, cap), 1) + s * cap)
            acc[...] += dot(hit, resx[s].reshape(cap, part))

        @pl.when(i < owners)
        def _():
            s = source(slot_of(i))
            for p in range(1, mp_n):
                give_copy(i, p, s, m).start()
            resx[s, m] = resout[s, m]

        return carry

    lax.fori_loop(0, owners + 2, finish, 0)
    result[...] = acc[...].astype(bf16)


def shards(
    subs,
    voxels,
    window_ids,
    voxel_slots,
    window_counts,
    norm_gain,
    w_query_key,
    w_value,
    w_out,
    ffn_gain,
    w_up,
    w_down,
):
    groups = lax.axis_size("groups")
    owners = lax.axis_size(("space", "sub"))
    mp_n = lax.axis_size("mp")
    rows, width = voxels.shape
    part = width // mp_n
    unit = math.lcm(128, 16 * mp_n)
    cap = -(-(2 * rows // owners) // unit) * unit
    piece = cap // mp_n
    far = owners - subs
    dma = pltpu.SemaphoreType.DMA
    i32 = jnp.int32
    pieces = 3 * mp_n
    return pl.pallas_call(
        functools.partial(block_kernel, groups, owners // subs, subs, mp_n),
        out_shape=jax.ShapeDtypeStruct((rows, part), bf16),
        in_specs=[SMEM] + [VMEM] * 4 + [ANY] * 5,
        out_specs=VMEM,
        scratch_shapes=[
            pltpu.VMEM((rows, width), bf16),
            pltpu.VMEM((1, rows), i32),
            pltpu.VMEM((rows, 128), i32),
            pltpu.VMEM((8, rows), bf16),
            pltpu.VMEM((far, cap, part), bf16),
            pltpu.VMEM((subs, mp_n, cap, part), bf16),
            pltpu.VMEM((owners, mp_n, cap, part), bf16),
            pltpu.VMEM((owners, 1, cap), i32),
            pltpu.VMEM((owners, 1, cap), i32),
            pltpu.VMEM((owners, cap, 128), i32),
            pltpu.VMEM((SLOTS, width), bf16),
            pltpu.VMEM(w_query_key.shape, bf16),
            pltpu.VMEM(w_value.shape, bf16),
            pltpu.VMEM((SLOTS, part), bf16),
            pltpu.VMEM((cap, part), f32),
            pltpu.VMEM((owners, mp_n, piece, part), bf16),
            pltpu.VMEM((mp_n, owners, piece, part), bf16),
            pltpu.VMEM((owners, piece, width), bf16),
            pltpu.VMEM((owners, mp_n, piece, part), bf16),
            pltpu.VMEM((owners, mp_n, piece, part), bf16),
            pltpu.VMEM((rows, part), f32),
            pltpu.VMEM((piece, width), f32),
            pltpu.VMEM((mp_n,) + w_out.shape, bf16),
            pltpu.VMEM((mp_n,) + w_up.shape, bf16),
            pltpu.VMEM((mp_n,) + w_down.shape, bf16),
            dma((far * mp_n,)), dma((far * mp_n,)), dma((subs,)), dma((subs,)),
            dma((owners,)), dma((owners,)),
            dma((far * mp_n * mp_n,)), dma((far * mp_n * mp_n,)),
            dma((owners * mp_n,)), dma((owners * mp_n,)),
            dma((owners * mp_n,)), dma((owners * mp_n,)),
            dma((pieces,)), dma((pieces,)),
            dma((pieces * groups * subs,)), dma((pieces * groups * subs,)),
            dma((5,)),
        ],
        compiler_params=pltpu.CompilerParams(
            collective_id=0, has_side_effects=True, vmem_limit_bytes=62 * 1024 * 1024
        ),
        name="block",
    )(
        window_counts, (window_ids * WLEN + voxel_slots).reshape(rows // 128, 128), norm_gain[None, :],
        ffn_gain[None, :], voxels, w_query_key, w_value, w_out, w_up, w_down,
    )


def solution(mesh):
    return jax.shard_map(
        functools.partial(shards, mesh.shape["sub"]),
        mesh=mesh,
        in_specs=(
            P(("groups", "space", "sub"), None),
            P(("groups", "space", "sub")),
            P(("groups", "space", "sub")),
            P("groups"),
            P(),
            P(None, None, "mp"),
            P(None, "mp"),
            P("mp", None),
            P(),
            P(None, "mp"),
            P("mp", None),
        ),
        out_specs=P(("groups", "space", "sub"), "mp"),
        check_vma=False,
    )
```
